32 devices in a mesh: dp: 4 (over x, core), mp: 8 (over z, y).
Axes of the slice: x: 2, y: 2, z: 4, core: 2. Of those that a mesh axis runs over, the one named last changes fastest.
Arguments:
- tokens: bfloat16 [3072, 6144], P('dp'), may hold values from -60 to 60
- ln_gain: float32 [6144], replicated, may hold values from 0.1 to 1.9
- w_qkv: bfloat16 [6144, 3, 6144], P('dp', None, 'mp'), may hold values from -1 to 1
- q_gain: float32 [128], replicated, may hold values from 0.7 to 2
- k_gain: float32 [128], replicated, may hold values from 0.7 to 2
Outputs:
- context: bfloat16 [3072, 6144], P('dp', 'mp')
The draws below stay inside these ranges and needn't reach their ends.
All inputs are finite; a program needn't handle non-finite values.
Results may differ from the reference program's by a relative error of at most 0.012.
The reference program's roundings to bfloat16 on the way count: a program that leaves them out, or rounds other values in their place, can miss the bound.
Values may be sent and summed in bfloat16 or wider, within the bound.
No kernel may reach another device: no remote copies, remote signals or barrier semaphores. Data moves between devices by JAX's collectives and lax.ppermute only.
A program may use at most 128 MiB of HBM per device.

```python
import jax
import jax.numpy as jnp
from jax import lax

D = 6144
HEADS = 48
HEAD_DIM = 128
PATCHES = 256
SPLITS = 4
IMAGES = 12
TOKENS = 3072


def draw_tokens(key, part):
    subkeys = jax.random.split(key, 3)
    row_scale = jnp.exp(jax.random.uniform(subkeys[0], (TOKENS, 1), jnp.float32, -1.2, 1.2))
    col_scale = jnp.exp(jax.random.uniform(subkeys[1], (1, D), jnp.float32, -1.2, 1.2))
    base_draw = jnp.clip(jax.random.normal(subkeys[2], (TOKENS, D), jnp.float32), -4.0, 4.0)
    values = base_draw * row_scale * col_scale
    return jnp.clip(values, -60.0, 60.0).astype(jnp.bfloat16)


def draw_w_qkv(key, part):
    subkeys = jax.random.split(key, 2)
    col_scale = jnp.exp(jax.random.uniform(subkeys[0], (1, 3, D), jnp.float32, -1.0, 1.2))
    base_draw = jnp.clip(jax.random.normal(subkeys[1], (D, 3, D), jnp.float32), -4.0, 4.0)
    values = base_draw * col_scale * D ** (-0.5)
    return jnp.clip(values, -1.0, 1.0).astype(jnp.bfloat16)


def setup_inputs(seed: int = 0) -> dict:
    key_of = jax.random.split(jax.random.key(seed), 6)
    tokens = draw_tokens(jax.random.fold_in(key_of[5], 71), 0)
    ln_gain = jnp.clip(1.0 + 0.18 * jax.random.normal(key_of[1], (D,), jnp.float32), 0.1, 1.9)
    w_qkv = draw_w_qkv(jax.random.fold_in(key_of[5], 71), 0)
    q_gain = jnp.clip(jax.random.uniform(key_of[3], (HEAD_DIM,), jnp.float32, 0.7, 2.0), 0.7, 2.0)
    k_gain = jnp.clip(jax.random.uniform(key_of[4], (HEAD_DIM,), jnp.float32, 0.7, 2.0), 0.7, 2.0)
    return {"tokens": tokens, "ln_gain": ln_gain, "w_qkv": w_qkv, "q_gain": q_gain, "k_gain": k_gain}


norm_eps = 1e-06

def layer_norm(values, gain_vector):
    centre = lax.optimization_barrier(jnp.mean(values, axis=-1, keepdims=True))
    centred = values - centre
    spread = lax.optimization_barrier(jnp.mean(centred * centred, axis=-1, keepdims=True))
    return centred * lax.rsqrt(spread + norm_eps) * gain_vector

def to_heads(features):
    leading = features.shape[:-1]
    parted = features.reshape(leading + (SPLITS, HEADS, HEAD_DIM // SPLITS))
    swapped = jnp.moveaxis(parted, -3, -2)
    return swapped.reshape(leading + (HEADS, HEAD_DIM))

def from_heads(features):
    leading = features.shape[:-2]
    parted = features.reshape(leading + (HEADS, SPLITS, HEAD_DIM // SPLITS))
    swapped = jnp.moveaxis(parted, -2, -3)
    return swapped.reshape(leading + (D,))

def reference(tokens, ln_gain, w_qkv, q_gain, k_gain):
    normed = layer_norm(tokens.astype(jnp.float32), ln_gain).astype(jnp.bfloat16)
    projected = jnp.dot(normed, w_qkv.reshape(D, 3 * D), preferred_element_type=jnp.float32).astype(jnp.bfloat16)
    projected = projected.reshape(IMAGES, PATCHES, 3, D)

    def attend(one_image):
        per_head = to_heads(one_image)
        queries = (layer_norm(per_head[:, 0].astype(jnp.float32), q_gain) * HEAD_DIM ** (-0.5)).astype(jnp.bfloat16)
        key_vecs = layer_norm(per_head[:, 1].astype(jnp.float32), k_gain).astype(jnp.bfloat16)
        values = per_head[:, 2]
        scores = jnp.einsum('qhe,khe->hqk', queries.astype(jnp.float32), key_vecs.astype(jnp.float32))
        raised = jnp.exp(scores)
        weights = (raised / lax.optimization_barrier(jnp.sum(raised, axis=-1, keepdims=True))).astype(jnp.bfloat16)
        attended = jnp.einsum('hqk,khe->qhe', weights.astype(jnp.float32), values.astype(jnp.float32)).astype(jnp.bfloat16)
        return from_heads(attended)
    context = lax.map(attend, projected)
    return context.reshape(TOKENS, D)
```

```python
import functools

import jax
import jax.numpy as jnp
from jax import lax
from jax.experimental import pallas as pl
from jax.experimental.pallas import tpu as pltpu
from jax.sharding import PartitionSpec as P


HEADS = 48
HEAD_DIM = 128
PATCHES = 256
SPLITS = 4
LANES = 128


norm_eps = 1e-06


def from_behind(shard, axis, by):
    length = lax.axis_size(axis)
    return lax.ppermute(shard, axis, [(i, (i + by) % length) for i in range(length)])


def layer_norm(values, gain_vector):
    centre = jnp.mean(values, axis=-1, keepdims=True)
    centred = values - centre
    spread = jnp.mean(centred * centred, axis=-1, keepdims=True)
    return centred * lax.rsqrt(spread + norm_eps) * gain_vector


def head_norm(pieces, gain_rows):
    values = pieces.astype(jnp.float32)
    centre = jnp.mean(values, axis=(0, 4), keepdims=True)
    centred = values - centre
    spread = jnp.mean(centred * centred, axis=(0, 4), keepdims=True)
    return centred * lax.rsqrt(spread + norm_eps) * gain_rows[:, None, None, None, :]


def ordered_gains(gain_vector, quarter_order):
    gain_table = gain_vector.reshape(SPLITS, -1)
    selector = (quarter_order[:, None] == jnp.arange(SPLITS, dtype=jnp.int32)[None, :]).astype(
        jnp.float32
    )
    return jnp.dot(selector, gain_table, precision=lax.Precision.HIGHEST)


def row_body(tokens, ln_gain, w_qkv, q_gain, k_gain):
    local_rows = tokens.shape[0]
    normed = layer_norm(tokens.astype(jnp.float32), ln_gain).astype(jnp.bfloat16)
    flat_weight = w_qkv.reshape(w_qkv.shape[0], -1)
    out_width = flat_weight.shape[1]
    row_piece = lax.all_gather(w_qkv, "dp", axis=0, tiled=True)
    partial_value = jnp.dot(
        normed, row_piece.reshape(row_piece.shape[0], out_width), preferred_element_type=jnp.float32
    )
    projected = partial_value.astype(jnp.bfloat16)
    groups = lax.axis_size("mp") // SPLITS
    head_count = HEADS // groups
    quarter_rows = PATCHES // SPLITS
    my_quarter = lax.axis_index("mp") // groups
    images = local_rows // PATCHES
    head_view = projected.reshape(images, PATCHES, 3, head_count, HEAD_DIM // SPLITS)
    queries = head_view[:, :, 0]
    keys_vals = head_view[:, :, 1:]
    counting = jnp.arange(SPLITS, dtype=jnp.int32)
    own_rows = lax.dynamic_slice_in_dim(queries, my_quarter * quarter_rows, quarter_rows, 1)
    query_list = [own_rows]
    pair_list = [keys_vals]
    for offset in range(1, SPLITS):
        outgoing = lax.dynamic_slice_in_dim(
            queries, (my_quarter + offset) % SPLITS * quarter_rows, quarter_rows, 1
        )
        got_query, got_pair = from_behind((outgoing, keys_vals), "mp", offset * groups)
        query_list.append(got_query)
        pair_list.append(got_pair)
    query_pieces = jnp.stack(query_list, 0)
    pair_pieces = jnp.stack(pair_list, 0)
    quarter_order = (my_quarter - counting) % SPLITS
    query_normed = (
        head_norm(query_pieces, ordered_gains(q_gain, quarter_order)) * HEAD_DIM ** (-0.5)
    ).astype(jnp.bfloat16)
    key_normed = head_norm(pair_pieces[:, :, :, 0], ordered_gains(k_gain, quarter_order)).astype(
        jnp.bfloat16
    )
    value_part = pair_pieces[:, :, :, 1]
    scores = jnp.einsum(
        "sirhe,sikhe->ihrk", query_normed, key_normed, preferred_element_type=jnp.float32
    )
    raised = jnp.exp(scores)
    weights = (raised / jnp.sum(raised, axis=-1, keepdims=True)).astype(jnp.bfloat16)
    context = jnp.einsum(
        "ihrk,sikhe->sirhe", weights, value_part, preferred_element_type=jnp.float32
    ).astype(jnp.bfloat16)
    rows_list = [context[0]]
    for offset in range(1, SPLITS):
        wanted = (my_quarter - offset) % SPLITS
        slot_index = jnp.sum(jnp.where(quarter_order == wanted, counting, 0))
        outgoing = lax.dynamic_index_in_dim(context, slot_index, 0, keepdims=False)
        rows_list.append(from_behind(outgoing, "mp", (SPLITS - offset) * groups))
    own_block = jnp.roll(jnp.concatenate(rows_list, 1), my_quarter * quarter_rows, axis=1)
    return own_block.reshape(local_rows, -1)


def swap(value, axis, mask):
    length = lax.axis_size(axis)
    return lax.ppermute(value, axis, [(i, i ^ mask) for i in range(length)])


def call(kernel, grid, in_specs, out_specs, out_shape, flops, bytes_accessed, scalars, scratch=()):
    return pl.pallas_call(
        kernel,
        grid_spec=pltpu.PrefetchScalarGridSpec(
            num_scalar_prefetch=scalars,
            grid=grid,
            in_specs=in_specs,
            out_specs=out_specs,
            scratch_shapes=list(scratch),
        ),
        out_shape=out_shape,
        cost_estimate=pl.CostEstimate(
            flops=flops, bytes_accessed=bytes_accessed, transcendentals=0
        ),
        compiler_params=pltpu.CompilerParams(
            dimension_semantics=("arbitrary",) * len(grid), vmem_limit_bytes=48 * 2**20
        ),
    )


def norm_kernel(parts, place, tokens, gain, out):
    width = tokens.shape[1] // parts
    values = tokens[...].astype(jnp.float32)
    centre = jnp.mean(values, axis=-1, keepdims=True)
    centred = values - centre
    spread = jnp.mean(centred * centred, axis=-1, keepdims=True)
    scale = lax.rsqrt(spread + norm_eps)
    for rel in range(parts):
        start = pl.multiple_of((place[0] ^ rel) * width, LANES)
        piece = tokens[:, pl.ds(start, width)].astype(jnp.float32)
        piece = (piece - centre) * scale * gain[:, pl.ds(start, width)]
        out[:, rel * width : (rel + 1) * width] = piece.astype(jnp.bfloat16)


def norm_tokens(place, tokens, gain, parts):
    rows, width = tokens.shape
    block = rows // 6
    return call(
        functools.partial(norm_kernel, parts),
        (rows // block,),
        [
            pl.BlockSpec((block, width), lambda i, s: (i, 0)),
            pl.BlockSpec((1, width), lambda i, s: (0, 0)),
        ],
        pl.BlockSpec((block, width), lambda i, s: (i, 0)),
        jax.ShapeDtypeStruct((rows, width), jnp.bfloat16),
        rows * width * 1200,
        rows * width * 4,
        1,
    )(place, tokens, gain[None, :])


def wide(weight):
    return jnp.concatenate([weight[p] for p in range(weight.shape[0])], axis=1)


def product(normed, first, second):
    depth = first.shape[1]
    total = jnp.dot(normed[:, :depth], wide(first), preferred_element_type=jnp.float32)
    return total + jnp.dot(normed[:, depth:], wide(second), preferred_element_type=jnp.float32)


def near_kernel(normed, first, second, out):
    out[...] = product(normed, first, second)


def near_product(normed, first, second, chunk):
    rows, width = normed.shape
    kinds, depth, _ = first.shape
    cols = kinds * LANES
    return call(
        near_kernel,
        (rows // PATCHES,),
        [
            pl.BlockSpec((PATCHES, width // 2), lambda i: (i, 0)),
            pl.BlockSpec((kinds, depth, LANES), lambda i: (0, 0, chunk)),
            pl.BlockSpec((kinds, depth, LANES), lambda i: (0, 0, chunk)),
        ],
        pl.BlockSpec((PATCHES, cols), lambda i: (i, 0)),
        jax.ShapeDtypeStruct((rows, cols), jnp.float32),
        rows * width * cols,
        rows * width + 2 * cols * width // 2,
        0,
    )(normed, first, second)


def far_kernel(quarter, total, normed, first, second, out0, out1, out2, out3, hold):
    done = (total[...] + product(normed, first, second)).astype(jnp.bfloat16)
    part = hold.shape[1] // SPLITS
    for kind in range(hold.shape[0]):
        hold[kind] = done[:, kind * LANES : (kind + 1) * LANES].T
    for rel, out in enumerate((out0, out1, out2, out3)):
        start = pl.multiple_of((quarter[0] ^ rel) * part, part)
        out[...] = hold[:, pl.ds(start, part), :]


def far_product(quarter, total, normed, first, second):
    rows, width = normed.shape
    kinds, depth, _ = first.shape
    cols = kinds * LANES
    part = LANES // SPLITS
    return call(
        far_kernel,
        (rows // PATCHES,),
        [
            pl.BlockSpec((PATCHES, cols), lambda i, s: (i, 0)),
            pl.BlockSpec((PATCHES, width // 2), lambda i, s: (i, 1)),
            pl.BlockSpec((kinds, depth, LANES), lambda i, s: (0, 0, 0)),
            pl.BlockSpec((kinds, depth, LANES), lambda i, s: (0, 0, 0)),
        ],
        [pl.BlockSpec((kinds, part, PATCHES), lambda i, s: (0, 0, i))] * SPLITS,
        [jax.ShapeDtypeStruct((kinds, part, rows), jnp.bfloat16)] * SPLITS,
        rows * width * cols,
        rows * width + 2 * cols * width // 2,
        1,
        [pltpu.VMEM((kinds, LANES, PATCHES), jnp.bfloat16)],
    )(quarter, total, normed, first, second)


def head_layer_norm(values, gain_rows):
    centre = jnp.mean(values, axis=0, keepdims=True)
    centred = values - centre
    spread = jnp.mean(centred * centred, axis=0, keepdims=True)
    return centred * lax.rsqrt(spread + norm_eps) * gain_rows


def attend_kernel(quarter, in0, in1, in2, in3, q_gain, k_gain, out0, out1, out2, out3):
    pieces = (in0, in1, in2, in3)
    part = in0.shape[1]

    def gains(ref):
        return jnp.concatenate(
            [
                ref[pl.ds(pl.multiple_of((quarter[0] ^ rel) * part, part), part), :]
                for rel in range(SPLITS)
            ],
            axis=0,
        )

    def features(kind):
        return jnp.concatenate([piece[kind] for piece in pieces], axis=0)

    query = head_layer_norm(features(0).astype(jnp.float32), gains(q_gain))
    query = (query * HEAD_DIM ** (-0.5)).astype(jnp.bfloat16)
    key = head_layer_norm(features(1).astype(jnp.float32), gains(k_gain)).astype(jnp.bfloat16)
    scores = lax.dot_general(
        key, query, (((0,), (0,)), ((), ())), preferred_element_type=jnp.float32
    )
    raised = jnp.exp(scores)
    weights = (raised / jnp.sum(raised, axis=0, keepdims=True)).astype(jnp.bfloat16)
    attended = jnp.dot(features(2), weights, preferred_element_type=jnp.float32)
    attended = attended.astype(jnp.bfloat16)
    for rel, out in enumerate((out0, out1, out2, out3)):
        out[...] = attended[rel * part : (rel + 1) * part]


def attend(quarter, pieces, q_gain, k_gain):
    kinds, part, rows = pieces[0].shape
    gain_spec = pl.BlockSpec((HEAD_DIM, PATCHES), lambda i, s: (0, 0))
    return call(
        attend_kernel,
        (rows // PATCHES,),
        [pl.BlockSpec((kinds, part, PATCHES), lambda i, s: (0, 0, i))] * SPLITS
        + [gain_spec, gain_spec],
        [pl.BlockSpec((part, PATCHES), lambda i, s: (0, i))] * SPLITS,
        [jax.ShapeDtypeStruct((part, rows), jnp.bfloat16)] * SPLITS,
        rows * PATCHES * HEAD_DIM * 30,
        rows * HEAD_DIM * 8,
        1,
    )(quarter, *pieces, q_gain, k_gain)


def finish_kernel(quarter, *refs):
    out, hold = refs[-2:]
    pieces = refs[:-2]
    part = pieces[0].shape[0]
    for chunk in range(len(pieces) // SPLITS):
        for rel in range(SPLITS):
            start = pl.multiple_of((quarter[0] ^ rel) * part, part)
            hold[pl.ds(start, part), :] = pieces[chunk * SPLITS + rel][...]
        out[:, chunk * LANES : (chunk + 1) * LANES] = hold[...].T


def finish(quarter, pieces):
    part, rows = pieces[0].shape
    width = part * len(pieces)
    return call(
        finish_kernel,
        (1,),
        [pl.BlockSpec((part, rows), lambda i, s: (0, 0))] * len(pieces),
        pl.BlockSpec((rows, width), lambda i, s: (0, 0)),
        jax.ShapeDtypeStruct((rows, width), jnp.bfloat16),
        rows * width * 100,
        rows * width * 4,
        1,
        [pltpu.VMEM((LANES, rows), jnp.bfloat16)],
    )(quarter, *pieces)


def after(value, *others):
    return lax.optimization_barrier((value, *others))[0]


def chunked_body(tokens, ln_gain, w_qkv, q_gain, k_gain):
    parts = lax.axis_size("dp")
    groups = lax.axis_size("mp") // SPLITS
    place = lax.axis_index("dp").astype(jnp.int32)[None]
    quarter = (lax.axis_index("mp") // groups).astype(jnp.int32)[None]
    weight = jnp.transpose(w_qkv, (1, 0, 2))
    chunks = weight.shape[2] // LANES
    slices = [weight[:, :, :LANES]]
    rest = after(weight, slices[0])
    slices += [rest[:, :, c * LANES : (c + 1) * LANES] for c in range(1, chunks)]
    beside = [swap(slices[c], "dp", 2) for c in range(chunks)]
    paired = swap(after(weight, slices[1]), "dp", 1)
    normed = norm_tokens(place, tokens, ln_gain, parts)
    wide_q = jnp.broadcast_to(q_gain[:, None], (HEAD_DIM, PATCHES))
    wide_k = jnp.broadcast_to(k_gain[:, None], (HEAD_DIM, PATCHES))
    returned = []
    for c in range(chunks):
        total = near_product(normed, weight, paired, c)
        across = swap(beside[c], "dp", 1)
        pieces = far_product(quarter, total, normed, beside[c], across)
        moved = [pieces[0]] + [swap(pieces[rel], "mp", rel * groups) for rel in range(1, SPLITS)]
        results = attend(quarter, moved, wide_q, wide_k)
        returned += [results[0]] + [
            swap(results[rel], "mp", rel * groups)
            for rel in range(1, SPLITS)
        ]
    return finish(quarter, returned)


def body(tokens, ln_gain, w_qkv, q_gain, k_gain):
    pairs = lax.axis_size("dp") == 4
    whole = w_qkv.shape[2] % LANES == 0 and HEAD_DIM // SPLITS * SPLITS == LANES
    if pairs and whole:
        return chunked_body(tokens, ln_gain, w_qkv, q_gain, k_gain)
    return row_body(tokens, ln_gain, w_qkv, q_gain, k_gain)


def solution(mesh):
    return jax.shard_map(
        body,
        mesh=mesh,
        in_specs=(P("dp", None), P(), P("dp", None, "mp"), P(), P()),
        out_specs=P("dp", "mp"),
        check_vma=False,
    )
```

```python
import functools

import jax
import jax.numpy as jnp
from jax import lax
from jax.experimental import pallas as pl
from jax.experimental.pallas import tpu as pltpu
from jax.sharding import PartitionSpec as P


HEADS = 48
HEAD_DIM = 128
PATCHES = 256
SPLITS = 4
LANES = 128


norm_eps = 1e-06


def from_behind(shard, axis, by):
    length = lax.axis_size(axis)
    return lax.ppermute(shard, axis, [(i, (i + by) % length) for i in range(length)])


def layer_norm(values, gain_vector):
    centre = jnp.mean(values, axis=-1, keepdims=True)
    centred = values - centre
    spread = jnp.mean(centred * centred, axis=-1, keepdims=True)
    return centred * lax.rsqrt(spread + norm_eps) * gain_vector


def head_norm(pieces, gain_rows):
    values = pieces.astype(jnp.float32)
    centre = jnp.mean(values, axis=(0, 4), keepdims=True)
    centred = values - centre
    spread = jnp.mean(centred * centred, axis=(0, 4), keepdims=True)
    return centred * lax.rsqrt(spread + norm_eps) * gain_rows[:, None, None, None, :]


def ordered_gains(gain_vector, quarter_order):
    gain_table = gain_vector.reshape(SPLITS, -1)
    selector = (quarter_order[:, None] == jnp.arange(SPLITS, dtype=jnp.int32)[None, :]).astype(
        jnp.float32
    )
    return jnp.dot(selector, gain_table, precision=lax.Precision.HIGHEST)


def row_body(tokens, ln_gain, w_qkv, q_gain, k_gain):
    local_rows = tokens.shape[0]
    normed = layer_norm(tokens.astype(jnp.float32), ln_gain).astype(jnp.bfloat16)
    flat_weight = w_qkv.reshape(w_qkv.shape[0], -1)
    out_width = flat_weight.shape[1]
    row_piece = lax.all_gather(w_qkv, "dp", axis=0, tiled=True)
    partial_value = jnp.dot(
        normed, row_piece.reshape(row_piece.shape[0], out_width), preferred_element_type=jnp.float32
    )
    projected = partial_value.astype(jnp.bfloat16)
    groups = lax.axis_size("mp") // SPLITS
    head_count = HEADS // groups
    quarter_rows = PATCHES // SPLITS
    my_quarter = lax.axis_index("mp") // groups
    images = local_rows // PATCHES
    head_view = projected.reshape(images, PATCHES, 3, head_count, HEAD_DIM // SPLITS)
    queries = head_view[:, :, 0]
    keys_vals = head_view[:, :, 1:]
    counting = jnp.arange(SPLITS, dtype=jnp.int32)
    own_rows = lax.dynamic_slice_in_dim(queries, my_quarter * quarter_rows, quarter_rows, 1)
    query_list = [own_rows]
    pair_list = [keys_vals]
    for offset in range(1, SPLITS):
        outgoing = lax.dynamic_slice_in_dim(
            queries, (my_quarter + offset) % SPLITS * quarter_rows, quarter_rows, 1
        )
        got_query, got_pair = from_behind((outgoing, keys_vals), "mp", offset * groups)
        query_list.append(got_query)
        pair_list.append(got_pair)
    query_pieces = jnp.stack(query_list, 0)
    pair_pieces = jnp.stack(pair_list, 0)
    quarter_order = (my_quarter - counting) % SPLITS
    query_normed = (
        head_norm(query_pieces, ordered_gains(q_gain, quarter_order)) * HEAD_DIM ** (-0.5)
    ).astype(jnp.bfloat16)
    key_normed = head_norm(pair_pieces[:, :, :, 0], ordered_gains(k_gain, quarter_order)).astype(
        jnp.bfloat16
    )
    value_part = pair_pieces[:, :, :, 1]
    scores = jnp.einsum(
        "sirhe,sikhe->ihrk", query_normed, key_normed, preferred_element_type=jnp.float32
    )
    raised = jnp.exp(scores)
    weights = (raised / jnp.sum(raised, axis=-1, keepdims=True)).astype(jnp.bfloat16)
    context = jnp.einsum(
        "ihrk,sikhe->sirhe", weights, value_part, preferred_element_type=jnp.float32
    ).astype(jnp.bfloat16)
    rows_list = [context[0]]
    for offset in range(1, SPLITS):
        wanted = (my_quarter - offset) % SPLITS
        slot_index = jnp.sum(jnp.where(quarter_order == wanted, counting, 0))
        outgoing = lax.dynamic_index_in_dim(context, slot_index, 0, keepdims=False)
        rows_list.append(from_behind(outgoing, "mp", (SPLITS - offset) * groups))
    own_block = jnp.roll(jnp.concatenate(rows_list, 1), my_quarter * quarter_rows, axis=1)
    return own_block.reshape(local_rows, -1)


def swap(value, axis, mask):
    length = lax.axis_size(axis)
    return lax.ppermute(value, axis, [(i, i ^ mask) for i in range(length)])


def call(kernel, grid, in_specs, out_specs, out_shape, flops, bytes_accessed, scalars, scratch=()):
    return pl.pallas_call(
        kernel,
        grid_spec=pltpu.PrefetchScalarGridSpec(
            num_scalar_prefetch=scalars,
            grid=grid,
            in_specs=in_specs,
            out_specs=out_specs,
            scratch_shapes=list(scratch),
        ),
        out_shape=out_shape,
        cost_estimate=pl.CostEstimate(
            flops=flops, bytes_accessed=bytes_accessed, transcendentals=0
        ),
        compiler_params=pltpu.CompilerParams(
            dimension_semantics=("arbitrary",) * len(grid), vmem_limit_bytes=48 * 2**20
        ),
    )


def norm_kernel(parts, place, tokens, gain, out):
    rows, whole = tokens.shape
    width = whole // parts
    tile = 16

    def one(index, _):
        at = pl.ds(pl.multiple_of(index * tile, tile), tile)
        centre = jnp.mean(tokens[at, :].astype(jnp.float32), axis=-1, keepdims=True)
        centred = tokens[at, :].astype(jnp.float32) - centre
        spread = jnp.mean(centred * centred, axis=-1, keepdims=True)
        scale = lax.rsqrt(spread + norm_eps)
        for rel in range(parts):
            start = pl.multiple_of((place[0] ^ rel) * width, LANES)
            piece = tokens[at, pl.ds(start, width)].astype(jnp.float32)
            piece = (piece - centre) * scale * gain[:, pl.ds(start, width)]
            out[at, rel * width : (rel + 1) * width] = piece.astype(jnp.bfloat16)
        return 0

    lax.fori_loop(0, rows // tile, one, 0, unroll=4)


def norm_tokens(place, tokens, gain, parts):
    rows, width = tokens.shape
    block = rows // 6
    return call(
        functools.partial(norm_kernel, parts),
        (rows // block,),
        [
            pl.BlockSpec((block, width), lambda i, s: (i, 0)),
            pl.BlockSpec((1, width), lambda i, s: (0, 0)),
        ],
        pl.BlockSpec((block, width), lambda i, s: (i, 0)),
        jax.ShapeDtypeStruct((rows, width), jnp.bfloat16),
        rows * width * 1200,
        rows * width * 4,
        1,
    )(place, tokens, gain[None, :])


def wide(weight):
    return jnp.concatenate([weight[p] for p in range(weight.shape[0])], axis=1)


STEPS = 2
SLOTS = 3


def multiply(normed, weights, first, chunk, near, skip, total, rows_in, cols_in, sems):
    parts = len(weights)
    kinds, block, lanes = cols_in.shape[1:]
    steps = parts * STEPS
    ahead = SLOTS - 1

    def row_copy(step, slot):
        at = pl.ds(pl.multiple_of((step + skip * STEPS) * block, LANES), block)
        return pltpu.make_async_copy(normed.at[:, at], rows_in.at[slot], sems.at[0, slot])

    def col_copy(rel, step, slot):
        at = pl.ds(pl.multiple_of((step - rel * STEPS) * block, LANES), block)
        kind, lane = (first, chunk * LANES) if rel < near else (0, 0)
        source = weights[rel].at[pl.ds(kind, kinds), at, pl.ds(lane, lanes)]
        return pltpu.make_async_copy(source, cols_in.at[slot], sems.at[1, slot])

    def fetch(step, slot):
        row_copy(step, slot).start()
        for rel in range(parts):

            @pl.when(step // STEPS == rel)
            def _():
                col_copy(rel, step, slot).start()

    def one(step, _):
        slot = step % SLOTS

        @pl.when(step + ahead < steps)
        def _():
            fetch(step + ahead, (step + ahead) % SLOTS)

        row_copy(step, slot).wait()
        col_copy(parts - 1, (parts - 1) * STEPS, slot).wait()
        total[...] += jnp.dot(
            rows_in[slot], wide(cols_in[slot]), preferred_element_type=jnp.float32
        )
        return 0

    for step in range(ahead):
        fetch(jnp.int32(step), step)
    lax.fori_loop(0, steps, one, 0)


def multiply_scratch(rows, depth, kinds, lanes):
    block = depth // STEPS
    return [
        pltpu.VMEM((SLOTS, rows, block), jnp.bfloat16),
        pltpu.VMEM((SLOTS, kinds, block, lanes), jnp.bfloat16),
        pltpu.SemaphoreType.DMA((2, SLOTS)),
    ]


def project_kernel(parts, near, skip, chunk, split, quarter, *refs):
    normed, weights = refs[0], refs[1 : parts + 1]
    head = parts + 1 + (skip > 0)
    outs, (total, hold, rows_in, cols_in, sems) = refs[head:-5], refs[-5:]
    total[...] = refs[parts + 1][...] if skip else jnp.zeros_like(total)
    multiply(normed, weights, 0, chunk, near, skip, total, rows_in, cols_in, sems)
    for kind in range(total.shape[1] // LANES):
        done = total[:, kind * LANES : (kind + 1) * LANES].astype(jnp.bfloat16)
        (hold if split else outs[0])[kind] = done.T
    if split:
        part = LANES // SPLITS
        for rel, out in enumerate(outs):
            start = pl.multiple_of((quarter[0] ^ rel) * part, part)
            out[...] = hold[:, pl.ds(start, part), :]


def project(quarter, normed, near, far, chunk, split, begun):
    rows, _ = normed.shape
    skip = 0 if begun is None else len(near)
    weights = far if skip else near + far
    kinds, depth, _ = far[0].shape
    cols = kinds * LANES
    part = LANES // SPLITS if split else LANES
    count = SPLITS if split else 1
    total_spec = [pl.BlockSpec((rows, cols), lambda i, s: (0, 0))] if skip else []
    kernel = functools.partial(
        project_kernel, len(weights), len(weights) - len(far), skip, chunk, split
    )
    return call(
        kernel,
        (1,),
        [pl.BlockSpec(memory_space=pltpu.HBM)] * (len(weights) + 1) + total_spec,
        [pl.BlockSpec((kinds, part, rows), lambda i, s: (0, 0, 0))] * count,
        [jax.ShapeDtypeStruct((kinds, part, rows), jnp.bfloat16)] * count,
        2 * rows * len(weights) * depth * cols,
        2 * (rows + cols) * len(weights) * depth,
        1,
        [
            pltpu.VMEM((rows, cols), jnp.float32),
            pltpu.VMEM((kinds, LANES, rows), jnp.bfloat16),
        ]
        + multiply_scratch(rows, depth, kinds, LANES),
    )(quarter, normed, *weights, *([begun] if skip else []))


def near_kernel(parts, first, chunk, normed, *refs):
    weights, (out, total, rows_in, cols_in, sems) = refs[:parts], refs[parts:]
    total[...] = jnp.zeros_like(total)
    multiply(normed, weights, first, chunk, parts, 0, total, rows_in, cols_in, sems)
    out[...] = total[...]


def near_sums(normed, near, name, chunk, count):
    rows, _ = normed.shape
    parts = len(near)
    first, last = UNIT_KINDS[name]
    depth = near[0].shape[1]
    cols = (last - first) * count * LANES
    return call(
        functools.partial(near_kernel, parts, first, chunk),
        (1,),
        [pl.BlockSpec(memory_space=pltpu.HBM)] * (parts + 1),
        pl.BlockSpec((rows, cols), lambda i: (0, 0)),
        jax.ShapeDtypeStruct((rows, cols), jnp.float32),
        2 * rows * parts * depth * cols,
        2 * (rows + cols) * parts * depth,
        0,
        [pltpu.VMEM((rows, cols), jnp.float32)]
        + multiply_scratch(rows, depth, last - first, count * LANES),
    )(normed, *near)


def tail_kernel(total, normed, first, second, *refs):
    shares, out = refs[:-1], refs[-1]
    depth = first.shape[1]
    value = total[...]
    value += jnp.dot(normed[:, :depth], first[0], preferred_element_type=jnp.float32)
    value += jnp.dot(normed[:, depth:], second[0], preferred_element_type=jnp.float32)
    value = value.astype(jnp.bfloat16).T
    part = LANES // SPLITS
    for index, weights in enumerate(shares):
        attended = []
        for head in range(SPLITS):
            at = index * LANES + head * part
            term = jnp.dot(
                value[at : at + part], weights[head], preferred_element_type=jnp.float32
            )
            attended.append(term.astype(jnp.bfloat16))
        out[:, index * LANES : (index + 1) * LANES] = jnp.concatenate(attended, axis=0).T


def tail(total, normed, first, second, *shares):
    rows, width = normed.shape
    depth = first.shape[1]
    cols = len(shares) * LANES
    return call(
        tail_kernel,
        (rows // PATCHES,),
        [
            pl.BlockSpec((PATCHES, cols), lambda i: (i, 0)),
            pl.BlockSpec((PATCHES, width // 2), lambda i: (i, 1)),
            pl.BlockSpec((1, depth, cols), lambda i: (0, 0, 0)),
            pl.BlockSpec((1, depth, cols), lambda i: (0, 0, 0)),
        ]
        + [pl.BlockSpec((SPLITS, PATCHES, PATCHES), lambda i: (0, 0, i))] * len(shares),
        pl.BlockSpec((PATCHES, cols), lambda i: (i, 0)),
        jax.ShapeDtypeStruct((rows, cols), jnp.bfloat16),
        rows * width * cols,
        rows * width + width * cols,
        0,
    )(total, normed, first, second, *shares)


def head_layer_norm(values, gain_rows):
    centre = jnp.mean(values, axis=0, keepdims=True)
    centred = values - centre
    spread = jnp.mean(centred * centred, axis=0, keepdims=True)
    return centred * lax.rsqrt(spread + norm_eps) * gain_rows


def softmax_of(query, key, q_rows, k_rows):
    query = head_layer_norm(query.astype(jnp.float32), q_rows)
    query = (query * HEAD_DIM ** (-0.5)).astype(jnp.bfloat16)
    key = head_layer_norm(key.astype(jnp.float32), k_rows).astype(jnp.bfloat16)
    scores = lax.dot_general(
        key, query, (((0,), (0,)), ((), ())), preferred_element_type=jnp.float32
    )
    raised = jnp.exp(scores)
    return (raised / jnp.sum(raised, axis=0, keepdims=True)).astype(jnp.bfloat16)


def gain_rows(quarter, ref):
    part = ref.shape[0] // SPLITS
    rows = []
    for rel in range(SPLITS):
        start = pl.multiple_of((quarter[0] ^ rel) * part, part)
        rows.append(ref[pl.ds(start, part), :])
    return jnp.concatenate(rows, axis=0)


def attend_kernel(quarter, *refs):
    pieces, (q_gain, k_gain), outs = refs[:SPLITS], refs[SPLITS : SPLITS + 2], refs[-SPLITS:]
    part = pieces[0].shape[1]
    query, key, value = (
        jnp.concatenate([piece[kind] for piece in pieces], axis=0) for kind in range(3)
    )
    weights = softmax_of(query, key, gain_rows(quarter, q_gain), gain_rows(quarter, k_gain))
    attended = jnp.dot(value, weights, preferred_element_type=jnp.float32)
    attended = attended.astype(jnp.bfloat16)
    for rel, out in enumerate(outs):
        out[...] = attended[rel * part : (rel + 1) * part]


def attend(quarter, pieces, q_gain, k_gain):
    kinds, part, rows = pieces[0].shape
    gain_spec = pl.BlockSpec((HEAD_DIM, PATCHES), lambda i, s: (0, 0))
    return call(
        attend_kernel,
        (rows // PATCHES,),
        [pl.BlockSpec((kinds, part, PATCHES), lambda i, s: (0, 0, i))] * SPLITS
        + [gain_spec, gain_spec],
        [pl.BlockSpec((part, PATCHES), lambda i, s: (0, i))] * SPLITS,
        [jax.ShapeDtypeStruct((part, rows), jnp.bfloat16)] * SPLITS,
        rows * PATCHES * HEAD_DIM * 30,
        rows * HEAD_DIM * 8,
        1,
    )(quarter, *pieces, q_gain, k_gain)


def weigh_kernel(quarter, *refs):
    pieces, (q_gain, k_gain), out = refs[:SPLITS], refs[SPLITS : SPLITS + 2], refs[-1]
    part = HEAD_DIM // SPLITS
    q_rows, k_rows = gain_rows(quarter, q_gain), gain_rows(quarter, k_gain)
    for head in range(SPLITS):
        query, key = (
            jnp.concatenate(
                [piece[kind, head * part : (head + 1) * part] for piece in pieces], axis=0
            )
            for kind in range(2)
        )
        out[head] = softmax_of(query, key, q_rows, k_rows)


def weigh(quarter, pieces, q_gain, k_gain):
    kinds, lanes, rows = pieces[0].shape
    gain_spec = pl.BlockSpec((HEAD_DIM, PATCHES), lambda i, s: (0, 0))
    return call(
        weigh_kernel,
        (rows // PATCHES,),
        [pl.BlockSpec((kinds, lanes, PATCHES), lambda i, s: (0, 0, i))] * SPLITS
        + [gain_spec, gain_spec],
        pl.BlockSpec((SPLITS, PATCHES, PATCHES), lambda i, s: (0, 0, i)),
        jax.ShapeDtypeStruct((SPLITS, PATCHES, rows), jnp.bfloat16),
        rows * PATCHES * HEAD_DIM * 80,
        rows * HEAD_DIM * 32,
        1,
    )(quarter, *pieces, q_gain, k_gain)


def finish_kernel(early, quarter, *refs):
    out, hold = refs[-2:]
    pieces, tails = refs[: early * SPLITS], refs[early * SPLITS : -2]
    part = pieces[0].shape[0]
    for chunk in range(early):
        for rel in range(SPLITS):
            start = pl.multiple_of((quarter[0] ^ rel) * part, part)
            hold[pl.ds(start, part), :] = pieces[chunk * SPLITS + rel][...]
        out[:, chunk * LANES : (chunk + 1) * LANES] = hold[...].T
    out[:, early * LANES :] = tails[0][...]


def finish(quarter, pieces, tails):
    part, rows = pieces[0].shape
    early = len(pieces) // SPLITS
    width = early * LANES + tails[0].shape[1]
    return call(
        functools.partial(finish_kernel, early),
        (1,),
        [pl.BlockSpec((part, rows), lambda i, s: (0, 0))] * len(pieces)
        + [pl.BlockSpec(tails[0].shape, lambda i, s: (0, 0))],
        pl.BlockSpec((rows, width), lambda i, s: (0, 0)),
        jax.ShapeDtypeStruct((rows, width), jnp.bfloat16),
        rows * width * 100,
        rows * width * 4,
        1,
        [pltpu.VMEM((LANES, rows), jnp.bfloat16)],
    )(quarter, *pieces, *tails)


def after(value, *others):
    return lax.optimization_barrier((value, *others))[0]


UNIT_KINDS = {"all": (0, 3), "pair": (0, 2), "value": (2, 3)}


def sequence(chunks):
    early = chunks - chunks // 2
    pairs = [("pair", c, 1) for c in range(early, chunks)]
    units = []
    for c in range(early - 1):
        units += [("all", c, 1)] + pairs[c : c + 1]
    units += pairs[early - 1 :] + [("all", early - 1, 1)]
    return units + [("value", early, chunks - early)]


def exchange(values, groups):
    return [values[0]] + [swap(values[rel], "mp", rel * groups) for rel in range(1, SPLITS)]


def gather(own, groups):
    beside = swap(own, "mp", groups)
    far = swap(own, "mp", 3 * groups)
    middle = swap(far, "mp", groups)
    return [own, beside, middle, far]


def cut_kernel(units, source, *outs):
    kind = pl.program_id(0)
    for (name, chunk, count), out in zip(units, outs):
        first, last = UNIT_KINDS[name]

        @pl.when((kind >= first) & (kind < last))
        def _():
            out[...] = source[:, :, chunk * LANES : (chunk + count) * LANES]


def cut(weight, units):
    kinds, depth, width = weight.shape
    blocks = 2
    block = depth // blocks

    def spec(name, _, count):
        first, last = UNIT_KINDS[name]

        def place(kind, index):
            at = jnp.where(kind < first, 0, jnp.where(kind < last, index, blocks - 1))
            return jnp.clip(kind - first, 0, last - first - 1), at, 0

        return pl.BlockSpec((1, block, count * LANES), place)

    def shape(name, _, count):
        first, last = UNIT_KINDS[name]
        return jax.ShapeDtypeStruct((last - first, depth, count * LANES), weight.dtype)

    return call(
        functools.partial(cut_kernel, units),
        (kinds, blocks),
        [pl.BlockSpec((1, block, width), lambda kind, index: (kind, index, 0))],
        [spec(*unit) for unit in units],
        [shape(*unit) for unit in units],
        weight.size * 500,
        weight.size * 4,
        0,
    )(weight)


def chunked_body(tokens, ln_gain, w_qkv, q_gain, k_gain):
    parts = lax.axis_size("dp")
    groups = lax.axis_size("mp") // SPLITS
    place = lax.axis_index("dp").astype(jnp.int32)[None]
    quarter = (lax.axis_index("mp") // groups).astype(jnp.int32)[None]
    weight = jnp.transpose(w_qkv, (1, 0, 2))
    units = sequence(weight.shape[2] // LANES)
    slices = [weight[:, :, :LANES]]
    slices += cut(after(weight, slices[0]), units[1:])
    beside = [swap(slices[n], "dp", 2) for n in range(len(units))]
    paired = swap(after(weight, slices[1]), "dp", 1)
    normed = norm_tokens(place, tokens, ln_gain, parts)
    wide_q = jnp.broadcast_to(q_gain[:, None], (HEAD_DIM, PATCHES))
    wide_k = jnp.broadcast_to(k_gain[:, None], (HEAD_DIM, PATCHES))
    near = (weight, paired)
    returned, tails, shares = [], [], []
    for n, (kind, chunk, count) in enumerate(units):
        across = swap(beside[n], "dp", 1)
        far = (beside[n], across)
        begun = None
        if n >= len(units) - 2:
            begun = near_sums(normed, near, kind, chunk, count)
        if kind == "value":
            tails.append(tail(begun, normed, *far, *shares))
            continue
        split = kind == "all"
        pieces = project(quarter, normed, near, far, chunk, split, begun)
        if split:
            moved = exchange(pieces, groups)
            results = attend(quarter, moved, wide_q, wide_k)
            returned += exchange(results, groups)
        else:
            moved = gather(pieces[0], groups)
            shares.append(weigh(quarter, moved, wide_q, wide_k))
    return finish(quarter, returned, tails)


def body(tokens, ln_gain, w_qkv, q_gain, k_gain):
    pairs = lax.axis_size("dp") == 4
    whole = w_qkv.shape[2] % LANES == 0 and HEAD_DIM // SPLITS * SPLITS == LANES
    if pairs and whole:
        return chunked_body(tokens, ln_gain, w_qkv, q_gain, k_gain)
    return row_body(tokens, ln_gain, w_qkv, q_gain, k_gain)


def solution(mesh):
    return jax.shard_map(
        body,
        mesh=mesh,
        in_specs=(P("dp", None), P(), P("dp", None, "mp"), P(), P()),
        out_specs=P("dp", "mp"),
        check_vma=False,
    )
```

```python
import functools

import jax
import jax.numpy as jnp
from jax import lax
from jax.experimental import pallas as pl
from jax.experimental.pallas import tpu as pltpu
from jax.sharding import PartitionSpec as P


HEADS = 48
HEAD_DIM = 128
PATCHES = 256
SPLITS = 4
LANES = 128


norm_eps = 1e-06


def from_behind(shard, axis, by):
    length = lax.axis_size(axis)
    return lax.ppermute(shard, axis, [(i, (i + by) % length) for i in range(length)])


def layer_norm(values, gain_vector):
    centre = jnp.mean(values, axis=-1, keepdims=True)
    centred = values - centre
    spread = jnp.mean(centred * centred, axis=-1, keepdims=True)
    return centred * lax.rsqrt(spread + norm_eps) * gain_vector


def head_norm(pieces, gain_rows):
    values = pieces.astype(jnp.float32)
    centre = jnp.mean(values, axis=(0, 4), keepdims=True)
    centred = values - centre
    spread = jnp.mean(centred * centred, axis=(0, 4), keepdims=True)
    return centred * lax.rsqrt(spread + norm_eps) * gain_rows[:, None, None, None, :]


def ordered_gains(gain_vector, quarter_order):
    gain_table = gain_vector.reshape(SPLITS, -1)
    selector = (quarter_order[:, None] == jnp.arange(SPLITS, dtype=jnp.int32)[None, :]).astype(
        jnp.float32
    )
    return jnp.dot(selector, gain_table, precision=lax.Precision.HIGHEST)


def row_body(tokens, ln_gain, w_qkv, q_gain, k_gain):
    local_rows = tokens.shape[0]
    normed = layer_norm(tokens.astype(jnp.float32), ln_gain).astype(jnp.bfloat16)
    flat_weight = w_qkv.reshape(w_qkv.shape[0], -1)
    out_width = flat_weight.shape[1]
    row_piece = lax.all_gather(w_qkv, "dp", axis=0, tiled=True)
    partial_value = jnp.dot(
        normed, row_piece.reshape(row_piece.shape[0], out_width), preferred_element_type=jnp.float32
    )
    projected = partial_value.astype(jnp.bfloat16)
    groups = lax.axis_size("mp") // SPLITS
    head_count = HEADS // groups
    quarter_rows = PATCHES // SPLITS
    my_quarter = lax.axis_index("mp") // groups
    images = local_rows // PATCHES
    head_view = projected.reshape(images, PATCHES, 3, head_count, HEAD_DIM // SPLITS)
    queries = head_view[:, :, 0]
    keys_vals = head_view[:, :, 1:]
    counting = jnp.arange(SPLITS, dtype=jnp.int32)
    own_rows = lax.dynamic_slice_in_dim(queries, my_quarter * quarter_rows, quarter_rows, 1)
    query_list = [own_rows]
    pair_list = [keys_vals]
    for offset in range(1, SPLITS):
        outgoing = lax.dynamic_slice_in_dim(
            queries, (my_quarter + offset) % SPLITS * quarter_rows, quarter_rows, 1
        )
        got_query, got_pair = from_behind((outgoing, keys_vals), "mp", offset * groups)
        query_list.append(got_query)
        pair_list.append(got_pair)
    query_pieces = jnp.stack(query_list, 0)
    pair_pieces = jnp.stack(pair_list, 0)
    quarter_order = (my_quarter - counting) % SPLITS
    query_normed = (
        head_norm(query_pieces, ordered_gains(q_gain, quarter_order)) * HEAD_DIM ** (-0.5)
    ).astype(jnp.bfloat16)
    key_normed = head_norm(pair_pieces[:, :, :, 0], ordered_gains(k_gain, quarter_order)).astype(
        jnp.bfloat16
    )
    value_part = pair_pieces[:, :, :, 1]
    scores = jnp.einsum(
        "sirhe,sikhe->ihrk", query_normed, key_normed, preferred_element_type=jnp.float32
    )
    raised = jnp.exp(scores)
    weights = (raised / jnp.sum(raised, axis=-1, keepdims=True)).astype(jnp.bfloat16)
    context = jnp.einsum(
        "ihrk,sikhe->sirhe", weights, value_part, preferred_element_type=jnp.float32
    ).astype(jnp.bfloat16)
    rows_list = [context[0]]
    for offset in range(1, SPLITS):
        wanted = (my_quarter - offset) % SPLITS
        slot_index = jnp.sum(jnp.where(quarter_order == wanted, counting, 0))
        outgoing = lax.dynamic_index_in_dim(context, slot_index, 0, keepdims=False)
        rows_list.append(from_behind(outgoing, "mp", (SPLITS - offset) * groups))
    own_block = jnp.roll(jnp.concatenate(rows_list, 1), my_quarter * quarter_rows, axis=1)
    return own_block.reshape(local_rows, -1)


def swap(value, axis, mask):
    length = lax.axis_size(axis)
    return lax.ppermute(value, axis, [(i, i ^ mask) for i in range(length)])


def call(kernel, grid, in_specs, out_specs, out_shape, flops, bytes_accessed, scalars, scratch=()):
    return pl.pallas_call(
        kernel,
        grid_spec=pltpu.PrefetchScalarGridSpec(
            num_scalar_prefetch=scalars,
            grid=grid,
            in_specs=in_specs,
            out_specs=out_specs,
            scratch_shapes=list(scratch),
        ),
        out_shape=out_shape,
        cost_estimate=pl.CostEstimate(
            flops=flops, bytes_accessed=bytes_accessed, transcendentals=0
        ),
        compiler_params=pltpu.CompilerParams(
            dimension_semantics=("arbitrary",) * len(grid), vmem_limit_bytes=43 * 2**20
        ),
    )


def norm_kernel(parts, place, tokens, gain, out):
    rows, whole = tokens.shape
    width = whole // parts
    tile = 16

    def one(index, _):
        at = pl.ds(pl.multiple_of(index * tile, tile), tile)
        centre = jnp.mean(tokens[at, :].astype(jnp.float32), axis=-1, keepdims=True)
        centred = tokens[at, :].astype(jnp.float32) - centre
        spread = jnp.mean(centred * centred, axis=-1, keepdims=True)
        scale = lax.rsqrt(spread + norm_eps)
        for rel in range(parts):
            start = pl.multiple_of((place[0] ^ rel) * width, LANES)
            piece = tokens[at, pl.ds(start, width)].astype(jnp.float32)
            piece = (piece - centre) * scale * gain[:, pl.ds(start, width)]
            out[at, rel * width : (rel + 1) * width] = piece.astype(jnp.bfloat16)
        return 0

    lax.fori_loop(0, rows // tile, one, 0, unroll=4)


def norm_tokens(place, tokens, gain, parts):
    rows, width = tokens.shape
    block = rows // 6
    return call(
        functools.partial(norm_kernel, parts),
        (rows // block,),
        [
            pl.BlockSpec((block, width), lambda i, s: (i, 0)),
            pl.BlockSpec((1, width), lambda i, s: (0, 0)),
        ],
        pl.BlockSpec((block, width), lambda i, s: (i, 0)),
        jax.ShapeDtypeStruct((rows, width), jnp.bfloat16),
        rows * width * 1200,
        rows * width * 4,
        1,
    )(place, tokens, gain[None, :])


def wide(weight):
    return jnp.concatenate([weight[p] for p in range(weight.shape[0])], axis=1)


STEPS = 2
SLOTS = 3


def multiply(normed, weights, first, chunk, near, skip, total, rows_in, cols_in, sems):
    parts = len(weights)
    kinds, block, lanes = cols_in.shape[1:]
    steps = parts * STEPS
    ahead = SLOTS - 1

    def row_copy(step, slot):
        at = pl.ds(pl.multiple_of((step + skip * STEPS) * block, LANES), block)
        return pltpu.make_async_copy(normed.at[:, at], rows_in.at[slot], sems.at[0, slot])

    def col_copy(rel, step, slot):
        at = pl.ds(pl.multiple_of((step - rel * STEPS) * block, LANES), block)
        kind, lane = (first, chunk * LANES) if rel < near else (0, 0)
        source = weights[rel].at[pl.ds(kind, kinds), at, pl.ds(lane, lanes)]
        return pltpu.make_async_copy(source, cols_in.at[slot], sems.at[1, slot])

    def fetch(step, slot):
        row_copy(step, slot).start()
        for rel in range(parts):

            @pl.when(step // STEPS == rel)
            def _():
                col_copy(rel, step, slot).start()

    def one(step, _):
        slot = step % SLOTS

        @pl.when(step + ahead < steps)
        def _():
            fetch(step + ahead, (step + ahead) % SLOTS)

        row_copy(step, slot).wait()
        col_copy(parts - 1, (parts - 1) * STEPS, slot).wait()
        total[...] += jnp.dot(
            rows_in[slot], wide(cols_in[slot]), preferred_element_type=jnp.float32
        )
        return 0

    for step in range(ahead):
        fetch(jnp.int32(step), step)
    lax.fori_loop(0, steps, one, 0)


def multiply_scratch(rows, depth, kinds, lanes):
    block = depth // STEPS
    return [
        pltpu.VMEM((SLOTS, rows, block), jnp.bfloat16),
        pltpu.VMEM((SLOTS, kinds, block, lanes), jnp.bfloat16),
        pltpu.SemaphoreType.DMA((2, SLOTS)),
    ]


def project_kernel(parts, near, skip, chunk, split, quarter, *refs):
    normed, weights = refs[0], refs[1 : parts + 1]
    head = parts + 1 + (skip > 0)
    outs, (total, hold, rows_in, cols_in, sems) = refs[head:-5], refs[-5:]
    total[...] = refs[parts + 1][...] if skip else jnp.zeros_like(total)
    multiply(normed, weights, 0, chunk, near, skip, total, rows_in, cols_in, sems)
    for kind in range(total.shape[1] // LANES):
        done = total[:, kind * LANES : (kind + 1) * LANES].astype(jnp.bfloat16)
        (hold if split else outs[0])[kind] = done.T
    if split:
        part = LANES // SPLITS
        for rel, out in enumerate(outs):
            start = pl.multiple_of((quarter[0] ^ rel) * part, part)
            out[...] = hold[:, pl.ds(start, part), :]


def project(quarter, normed, near, far, chunk, split, begun):
    rows, _ = normed.shape
    skip = 0 if begun is None else len(near)
    weights = far if skip else near + far
    kinds, depth, _ = far[0].shape
    cols = kinds * LANES
    part = LANES // SPLITS if split else LANES
    count = SPLITS if split else 1
    total_spec = [pl.BlockSpec((rows, cols), lambda i, s: (0, 0))] if skip else []
    kernel = functools.partial(
        project_kernel, len(weights), len(weights) - len(far), skip, chunk, split
    )
    return call(
        kernel,
        (1,),
        [pl.BlockSpec(memory_space=pltpu.HBM)] * (len(weights) + 1) + total_spec,
        [pl.BlockSpec((kinds, part, rows), lambda i, s: (0, 0, 0))] * count,
        [jax.ShapeDtypeStruct((kinds, part, rows), jnp.bfloat16)] * count,
        2 * rows * len(weights) * depth * cols,
        2 * (rows + cols) * len(weights) * depth,
        1,
        [
            pltpu.VMEM((rows, cols), jnp.float32),
            pltpu.VMEM((kinds, LANES, rows), jnp.bfloat16),
        ]
        + multiply_scratch(rows, depth, kinds, LANES),
    )(quarter, normed, *weights, *([begun] if skip else []))


def near_kernel(parts, first, chunk, normed, *refs):
    weights, (out, total, rows_in, cols_in, sems) = refs[:parts], refs[parts:]
    total[...] = jnp.zeros_like(total)
    multiply(normed, weights, first, chunk, parts, 0, total, rows_in, cols_in, sems)
    out[...] = total[...]


def near_sums(normed, near, name, chunk, count):
    rows, _ = normed.shape
    parts = len(near)
    first, last = UNIT_KINDS[name]
    depth = near[0].shape[1]
    cols = (last - first) * count * LANES
    return call(
        functools.partial(near_kernel, parts, first, chunk),
        (1,),
        [pl.BlockSpec(memory_space=pltpu.HBM)] * (parts + 1),
        pl.BlockSpec((rows, cols), lambda i: (0, 0)),
        jax.ShapeDtypeStruct((rows, cols), jnp.float32),
        2 * rows * parts * depth * cols,
        2 * (rows + cols) * parts * depth,
        0,
        [pltpu.VMEM((rows, cols), jnp.float32)]
        + multiply_scratch(rows, depth, last - first, count * LANES),
    )(normed, *near)


def tail_kernel(total, normed, first, second, *refs):
    shares, out = refs[:-1], refs[-1]
    depth = first.shape[1]
    value = total[...]
    value += jnp.dot(normed[:, :depth], first[0], preferred_element_type=jnp.float32)
    value += jnp.dot(normed[:, depth:], second[0], preferred_element_type=jnp.float32)
    value = value.astype(jnp.bfloat16).T
    part = LANES // SPLITS
    for index, weights in enumerate(shares):
        attended = []
        for head in range(SPLITS):
            at = index * LANES + head * part
            term = jnp.dot(
                value[at : at + part], weights[head], preferred_element_type=jnp.float32
            )
            attended.append(term.astype(jnp.bfloat16))
        out[:, index * LANES : (index + 1) * LANES] = jnp.concatenate(attended, axis=0).T


def tail(total, normed, first, second, skip, *shares):
    rows, width = normed.shape
    depth = first.shape[1]
    cols = len(shares) * LANES
    return call(
        tail_kernel,
        (rows // PATCHES,),
        [
            pl.BlockSpec((PATCHES, cols), lambda i: (i, skip // len(shares))),
            pl.BlockSpec((PATCHES, width // 2), lambda i: (i, 1)),
            pl.BlockSpec((1, depth, cols), lambda i: (0, 0, 0)),
            pl.BlockSpec((1, depth, cols), lambda i: (0, 0, 0)),
        ]
        + [pl.BlockSpec((SPLITS, PATCHES, PATCHES), lambda i: (0, 0, i))] * len(shares),
        pl.BlockSpec((PATCHES, cols), lambda i: (i, 0)),
        jax.ShapeDtypeStruct((rows, cols), jnp.bfloat16),
        rows * width * cols,
        rows * width + width * cols,
        0,
    )(total, normed, first, second, *shares)


def head_layer_norm(values, gain_rows):
    centre = jnp.mean(values, axis=0, keepdims=True)
    centred = values - centre
    spread = jnp.mean(centred * centred, axis=0, keepdims=True)
    return centred * lax.rsqrt(spread + norm_eps) * gain_rows


def softmax_of(query, key, q_rows, k_rows):
    query = head_layer_norm(query.astype(jnp.float32), q_rows)
    query = (query * HEAD_DIM ** (-0.5)).astype(jnp.bfloat16)
    key = head_layer_norm(key.astype(jnp.float32), k_rows).astype(jnp.bfloat16)
    scores = lax.dot_general(
        key, query, (((0,), (0,)), ((), ())), preferred_element_type=jnp.float32
    )
    raised = jnp.exp(scores)
    return (raised / jnp.sum(raised, axis=0, keepdims=True)).astype(jnp.bfloat16)


def gain_rows(quarter, ref):
    part = ref.shape[0] // SPLITS
    rows = []
    for rel in range(SPLITS):
        start = pl.multiple_of((quarter[0] ^ rel) * part, part)
        rows.append(ref[pl.ds(start, part), :])
    return jnp.concatenate(rows, axis=0)


def attend_kernel(quarter, *refs):
    pieces, (q_gain, k_gain), outs = refs[:SPLITS], refs[SPLITS : SPLITS + 2], refs[-SPLITS:]
    part = pieces[0].shape[1]
    query, key, value = (
        jnp.concatenate([piece[kind] for piece in pieces], axis=0) for kind in range(3)
    )
    weights = softmax_of(query, key, gain_rows(quarter, q_gain), gain_rows(quarter, k_gain))
    attended = jnp.dot(value, weights, preferred_element_type=jnp.float32)
    attended = attended.astype(jnp.bfloat16)
    for rel, out in enumerate(outs):
        out[...] = attended[rel * part : (rel + 1) * part]


def attend(quarter, pieces, q_gain, k_gain):
    kinds, part, rows = pieces[0].shape
    gain_spec = pl.BlockSpec((HEAD_DIM, PATCHES), lambda i, s: (0, 0))
    return call(
        attend_kernel,
        (rows // PATCHES,),
        [pl.BlockSpec((kinds, part, PATCHES), lambda i, s: (0, 0, i))] * SPLITS
        + [gain_spec, gain_spec],
        [pl.BlockSpec((part, PATCHES), lambda i, s: (0, i))] * SPLITS,
        [jax.ShapeDtypeStruct((part, rows), jnp.bfloat16)] * SPLITS,
        rows * PATCHES * HEAD_DIM * 30,
        rows * HEAD_DIM * 8,
        1,
    )(quarter, *pieces, q_gain, k_gain)


def weigh_kernel(quarter, *refs):
    pieces, (q_gain, k_gain), out = refs[:SPLITS], refs[SPLITS : SPLITS + 2], refs[-1]
    part = HEAD_DIM // SPLITS
    q_rows, k_rows = gain_rows(quarter, q_gain), gain_rows(quarter, k_gain)
    for head in range(SPLITS):
        query, key = (
            jnp.concatenate(
                [piece[kind, head * part : (head + 1) * part] for piece in pieces], axis=0
            )
            for kind in range(2)
        )
        out[head] = softmax_of(query, key, q_rows, k_rows)


def weigh(quarter, pieces, q_gain, k_gain):
    kinds, lanes, rows = pieces[0].shape
    gain_spec = pl.BlockSpec((HEAD_DIM, PATCHES), lambda i, s: (0, 0))
    return call(
        weigh_kernel,
        (rows // PATCHES,),
        [pl.BlockSpec((kinds, lanes, PATCHES), lambda i, s: (0, 0, i))] * SPLITS
        + [gain_spec, gain_spec],
        pl.BlockSpec((SPLITS, PATCHES, PATCHES), lambda i, s: (0, 0, i)),
        jax.ShapeDtypeStruct((SPLITS, PATCHES, rows), jnp.bfloat16),
        rows * PATCHES * HEAD_DIM * 80,
        rows * HEAD_DIM * 32,
        1,
    )(quarter, *pieces, q_gain, k_gain)


def finish_kernel(early, quarter, *refs):
    out, hold = refs[-2:]
    pieces, tails = refs[: early * SPLITS], refs[early * SPLITS : -2]
    part = pieces[0].shape[0]
    for chunk in range(early):
        for rel in range(SPLITS):
            start = pl.multiple_of((quarter[0] ^ rel) * part, part)
            hold[pl.ds(start, part), :] = pieces[chunk * SPLITS + rel][...]
        out[:, chunk * LANES : (chunk + 1) * LANES] = hold[...].T
    start = early * LANES
    for last in tails:
        out[:, start : start + last.shape[1]] = last[...]
        start += last.shape[1]


def finish(quarter, pieces, tails):
    part, rows = pieces[0].shape
    early = len(pieces) // SPLITS
    width = early * LANES + sum(last.shape[1] for last in tails)
    return call(
        functools.partial(finish_kernel, early),
        (1,),
        [pl.BlockSpec((part, rows), lambda i, s: (0, 0))] * len(pieces)
        + [pl.BlockSpec(last.shape, lambda i, s: (0, 0)) for last in tails],
        pl.BlockSpec((rows, width), lambda i, s: (0, 0)),
        jax.ShapeDtypeStruct((rows, width), jnp.bfloat16),
        rows * width * 100,
        rows * width * 4,
        1,
        [pltpu.VMEM((LANES, rows), jnp.bfloat16)],
    )(quarter, *pieces, *tails)


def after(value, *others):
    return lax.optimization_barrier((value, *others))[0]


UNIT_KINDS = {"all": (0, 3), "pair": (0, 2), "value": (2, 3)}


def sequence(chunks):
    early = chunks - chunks // 2
    pairs = [("pair", c, 1) for c in range(early, chunks)]
    units = pairs[:1]
    for c in range(early):
        units += pairs[c + 1 : c + 2] + [("all", c, 1)]
    most = max(chunks - early - 1, 1)
    units.append(("value", early, most))
    return units + [("value", c, 1) for c in range(early + most, chunks)]


def exchange(values, groups):
    return [values[0]] + [swap(values[rel], "mp", rel * groups) for rel in range(1, SPLITS)]


def gather(own, groups):
    beside = swap(own, "mp", groups)
    far = swap(own, "mp", 3 * groups)
    middle = swap(far, "mp", groups)
    return [own, beside, middle, far]


def cut_kernel(units, source, *outs):
    kind = pl.program_id(0)
    for (name, chunk, count), out in zip(units, outs):
        first, last = UNIT_KINDS[name]

        @pl.when((kind >= first) & (kind < last))
        def _():
            out[...] = source[:, :, chunk * LANES : (chunk + count) * LANES]


def cut(weight, units):
    kinds, depth, width = weight.shape
    blocks = 2
    block = depth // blocks

    def spec(name, _, count):
        first, last = UNIT_KINDS[name]

        def place(kind, index):
            at = jnp.where(kind < first, 0, jnp.where(kind < last, index, blocks - 1))
            return jnp.clip(kind - first, 0, last - first - 1), at, 0

        return pl.BlockSpec((1, block, count * LANES), place)

    def shape(name, _, count):
        first, last = UNIT_KINDS[name]
        return jax.ShapeDtypeStruct((last - first, depth, count * LANES), weight.dtype)

    return call(
        functools.partial(cut_kernel, units),
        (kinds, blocks),
        [pl.BlockSpec((1, block, width), lambda kind, index: (kind, index, 0))],
        [spec(*unit) for unit in units],
        [shape(*unit) for unit in units],
        weight.size * 500,
        weight.size * 4,
        0,
    )(weight)


def chunked_body(tokens, ln_gain, w_qkv, q_gain, k_gain):
    parts = lax.axis_size("dp")
    groups = lax.axis_size("mp") // SPLITS
    place = lax.axis_index("dp").astype(jnp.int32)[None]
    quarter = (lax.axis_index("mp") // groups).astype(jnp.int32)[None]
    weight = jnp.transpose(w_qkv, (1, 0, 2))
    units = sequence(weight.shape[2] // LANES)
    first, last = UNIT_KINDS[units[0][0]]
    start = units[0][1] * LANES
    slices = [weight[first:last, :, start : start + units[0][2] * LANES]]
    slices += cut(after(weight, slices[0]), units[1:])
    beside = [swap(slices[n], "dp", 2) for n in range(len(units))]
    paired = swap(after(weight, slices[1]), "dp", 1)
    normed = norm_tokens(place, tokens, ln_gain, parts)
    wide_q = jnp.broadcast_to(q_gain[:, None], (HEAD_DIM, PATCHES))
    wide_k = jnp.broadcast_to(k_gain[:, None], (HEAD_DIM, PATCHES))
    near = (weight, paired)
    returned, tails, shares = [], [], []
    for n, (kind, chunk, count) in enumerate(units):
        across = swap(beside[n], "dp", 1)
        far = (beside[n], across)
        if kind == "value":
            if not tails:
                late = sum(unit[2] for unit in units[n:])
                begun = near_sums(normed, near, kind, chunk, late)
            skip = chunk - (len(returned) // SPLITS)
            mine = shares[skip : skip + count]
            tails.append(tail(begun, normed, *far, skip, *mine))
            continue
        begun = None
        if units[n + 1][0] == "value":
            begun = near_sums(normed, near, kind, chunk, count)
        split = kind == "all"
        pieces = project(quarter, normed, near, far, chunk, split, begun)
        if split:
            moved = exchange(pieces, groups)
            results = attend(quarter, moved, wide_q, wide_k)
            returned += exchange(results, groups)
        else:
            moved = gather(pieces[0], groups)
            shares.append(weigh(quarter, moved, wide_q, wide_k))
    return finish(quarter, returned, tails)


def body(tokens, ln_gain, w_qkv, q_gain, k_gain):
    pairs = lax.axis_size("dp") == 4
    whole = w_qkv.shape[2] % LANES == 0 and HEAD_DIM // SPLITS * SPLITS == LANES
    if pairs and whole:
        return chunked_body(tokens, ln_gain, w_qkv, q_gain, k_gain)
    return row_body(tokens, ln_gain, w_qkv, q_gain, k_gain)


def solution(mesh):
    return jax.shard_map(
        body,
        mesh=mesh,
        in_specs=(P("dp", None), P(), P("dp", None, "mp"), P(), P()),
        out_specs=P("dp", "mp"),
        check_vma=False,
    )
```
